32 devices in a mesh: ma: 8 (over z, y), vert: 4 (over x, core).
Axes of the slice: x: 2, y: 2, z: 4, core: 2. Of those that a mesh axis runs over, the one named last changes fastest.
Arguments:
- trial_block: bfloat16 [128, 64, 4, 1024], P('vert', 'ma'), may hold values from -6 to 6
- legendre: bfloat16 [64, 2, 32, 1024], P('ma'), may hold values from -0.1875 to 0.1875
- order_slot: int32 [64], replicated, may hold values from 0 to 63, each once
- cycle_start: int32 [32], replicated, may hold values from 0 to 127
- cycle_count: int32 [32], replicated, may hold values from 0 to 128, as said below
- cycle_weight: float32 [32], replicated, may hold values from 4 to 32
Outputs:
- new_basis: bfloat16 [128, 64, 4, 1024], P('vert', 'ma')
- ritz_matrix: float32 [128, 128], replicated
The draws below stay inside these ranges and needn't reach their ends.
Inputs may be any that keep to these rules, and one draw needn't show every extreme that they name: `cycle_count`: exactly 8 consecutive cycles have a nonzero count, and one of them has 128.
All inputs are finite; a program needn't handle non-finite values.
Results may differ from the reference program's by a relative error of at most 0.0073.
The reference program's roundings to bfloat16 on the way (of `fields`, `weighted`, `returned`, `adjoint`, `applied` and `mixing`) count: a program that leaves them out, or rounds other values in their place, can miss the bound.
Values may be sent and summed in bfloat16 or wider, within the bound.
A program may use at most 192 MiB of HBM per device.

```python
import math
import jax
import jax.numpy as jnp
from jax import lax

LDEG = 1024
ORDERS = 64
CYCLES = 32
LIVE = 8
NLON = 128
K = 128
NC = 262144


def draw_cycle_count(key, part):
    keys = jax.random.split(jax.random.fold_in(key, 11), 3)
    band_start = jax.random.randint(keys[0], (), 0, CYCLES - LIVE + 1)
    counts = jax.random.randint(keys[1], (CYCLES,), 1, NLON + 1)
    full_cycle = jax.random.randint(keys[2], (), 0, LIVE)
    cycle_index = jnp.arange(CYCLES)
    inside = (cycle_index >= band_start) & (cycle_index < band_start + LIVE)
    counts = jnp.where(cycle_index == band_start + full_cycle, NLON, counts)
    return jnp.where(inside, counts, 0).astype(jnp.int32)


def set_ends(values, rng, smallest, high):
    index_at = [jax.random.randint(jax.random.fold_in(rng, axis), (), 0, length) for axis, length in enumerate(values.shape)]
    main_axis = values.shape.index(max(values.shape))
    next_to = index_at[:main_axis] + [(index_at[main_axis] + 1) % values.shape[main_axis]] + index_at[main_axis + 1:]
    return values.at[tuple(index_at)].set(smallest).at[tuple(next_to)].set(high)


def block_scale(key, shape, cuts, smallest, largest):
    loudness, own = 1.0, jax.random.fold_in(key, 6)
    for axis_at, parts in cuts:
        draws = jnp.exp(jax.random.uniform(jax.random.fold_in(own, axis_at), (parts,), jnp.float32, smallest / len(cuts), largest / len(cuts)))
        loudness = loudness * jnp.repeat(draws, shape[axis_at] // parts).reshape([-1 if axis == axis_at else 1 for axis in range(len(shape))])
    return loudness


def bell_draw(key, extent, width, limit, cuts=(), kind=jnp.bfloat16):
    array = width * jax.random.normal(key, extent, jnp.float32)
    if cuts:
        array = array * block_scale(key, extent, cuts, -0.22, 0.18)
    return jnp.clip(array, -limit, limit).astype(kind)


def setup_inputs(seed: int = 0) -> dict:
    key_list = jax.random.split(jax.random.key(seed), 7)
    return {
        "trial_block": bell_draw(key_list[0], (K, ORDERS, 4, LDEG), 1.0, 6.0, ((0, 4), (1, 8))),
        "legendre": bell_draw(key_list[1], (ORDERS, 2, CYCLES, LDEG), LDEG ** -0.5, 0.1875, ((0, 8),)),
        "order_slot": jax.random.permutation(key_list[2], ORDERS).astype(jnp.int32),
        "cycle_start": set_ends(jax.random.randint(key_list[3], (CYCLES,), 0, NLON), jax.random.fold_in(key_list[3], 1), 0, NLON - 1).astype(jnp.int32),
        "cycle_count": draw_cycle_count(jax.random.fold_in(key_list[6], 71), 0),
        "cycle_weight": jnp.clip(jnp.exp(jax.random.uniform(key_list[5], (CYCLES,), jnp.float32, math.log(4.0), math.log(32.0))), 4.0, 32.0),
    }


def combine_fields(products):
    first_kind = products[:, 0]
    second_kind = products[:, 1]
    return jnp.stack([first_kind[..., 0] + second_kind[..., 3], first_kind[..., 1] - second_kind[..., 2], second_kind[..., 1] - first_kind[..., 2], -second_kind[..., 0] - first_kind[..., 3]], axis=-1)

def adjoint_terms(returned):
    gtc = returned[..., 0]
    gts = returned[..., 1]
    gpc = returned[..., 2]
    gps = returned[..., 3]
    first_kind = jnp.stack([gtc, gts, -gpc, -gps], axis=-1)
    second_kind = jnp.stack([-gps, gpc, -gts, gtc], axis=-1)
    return jnp.stack([first_kind, second_kind], axis=1)

def fourier_tables(order_slot, longitudes, orders_total):
    longitude = jnp.arange(longitudes, dtype=jnp.int32)
    phases = longitude[:, None] * order_slot[None, :].astype(jnp.int32) % longitudes
    angles = phases.astype(jnp.float32) * (2.0 * math.pi / longitudes)
    scale = 1.0 / math.sqrt(orders_total)
    return ((jnp.cos(angles) * scale).astype(jnp.bfloat16), (jnp.sin(angles) * scale).astype(jnp.bfloat16))

def finish_ritz(gram_trial, cross, gram_applied):
    factor_trial = jnp.linalg.cholesky(gram_trial)
    half_solved = lax.linalg.triangular_solve(factor_trial, cross, left_side=True, lower=True)
    ritz_matrix = lax.linalg.triangular_solve(factor_trial, half_solved.T, left_side=True, lower=True).T
    factor_applied = jnp.linalg.cholesky(gram_applied)
    identity = jnp.eye(gram_applied.shape[0], dtype=gram_applied.dtype)
    mixing = lax.linalg.triangular_solve(factor_applied, identity, left_side=True, lower=True)
    return (ritz_matrix, mixing.astype(jnp.bfloat16))

def reference(trial_block, legendre, order_slot, cycle_start, cycle_count, cycle_weight):
    highest = lax.Precision.HIGHEST
    block = trial_block.astype(jnp.float32)
    table = legendre.astype(jnp.float32)
    products = lax.dot_general(table, block, (((3,), (3,)), ((0,), (1,))), precision=highest)
    fields = combine_fields(products).astype(jnp.bfloat16)
    cosine, sines = fourier_tables(order_slot, NLON, ORDERS)
    cosine_wide = cosine.astype(jnp.float32)
    sines_wide = sines.astype(jnp.float32)
    pieces = fields.astype(jnp.float32)
    grid_values = jnp.einsum('jo,orkc->rckj', cosine_wide, pieces[..., 0::2], precision=highest)
    grid_values = grid_values + jnp.einsum('jo,orkc->rckj', sines_wide, pieces[..., 1::2], precision=highest)
    longitude = jnp.arange(NLON, dtype=jnp.int32)
    inside = ((longitude[None, :] - cycle_start[:, None]) % NLON < cycle_count[:, None]).astype(jnp.float32)
    factor = inside * cycle_weight[:, None].astype(jnp.float32)
    weighted = (grid_values * factor[:, None, None, :]).astype(jnp.bfloat16).astype(jnp.float32)
    back_cos = jnp.einsum('jo,rckj->orkc', cosine_wide, weighted, precision=highest)
    back_sin = jnp.einsum('jo,rckj->orkc', sines_wide, weighted, precision=highest)
    returned = jnp.stack([back_cos[..., 0], back_sin[..., 0], back_cos[..., 1], back_sin[..., 1]], axis=-1).astype(jnp.bfloat16)
    adjoint = adjoint_terms(returned).astype(jnp.float32)
    adjoint = adjoint.reshape(ORDERS, 2, CYCLES, K * 4)
    applied = lax.dot_general(adjoint, table, (((1, 2), (1, 2)), ((0,), (0,))), precision=highest)
    applied = applied.reshape(ORDERS, K, 4, LDEG).transpose(1, 0, 2, 3).astype(jnp.bfloat16)
    trial_flat = trial_block.reshape(K, NC)
    applied_flat = applied.reshape(K, NC)
    gram_trial = jnp.dot(trial_flat.astype(jnp.float32), trial_flat.T.astype(jnp.float32), preferred_element_type=jnp.float32) / NC
    cross = jnp.dot(trial_flat.astype(jnp.float32), applied_flat.T.astype(jnp.float32), preferred_element_type=jnp.float32) / NC
    gram_applied = jnp.dot(applied_flat.astype(jnp.float32), applied_flat.T.astype(jnp.float32), preferred_element_type=jnp.float32) / NC
    ritz_matrix, mixing = finish_ritz(gram_trial, cross, gram_applied)
    new_basis = jnp.dot(mixing.astype(jnp.float32), applied_flat.astype(jnp.float32), preferred_element_type=jnp.float32)
    new_basis = new_basis.reshape(K, ORDERS, 4, LDEG).astype(jnp.bfloat16)
    return (new_basis, ritz_matrix)
```

```python
import functools
import math

import jax
import jax.numpy as jnp
from jax import lax
from jax.experimental import pallas as pl
from jax.experimental.pallas import tpu as pltpu
from jax.sharding import PartitionSpec as P

MESH = pl.DeviceIdType.MESH
VMEM = pltpu.VMEM
F32 = jnp.float32
BF16 = jnp.bfloat16
HIGHEST = lax.Precision.HIGHEST
GRANT = 60 * 1024 * 1024


def on_vmem(count):
    return [pl.BlockSpec(memory_space=VMEM)] * count


def transform_kernel(
    n_ma, n_vert, width, own_ref, table_ref, back_ref, factor_ref, out_ref,
    gathered, ma_send, ma_recv, vert_send, vert_recv,
):
    ma = lax.axis_index("ma")
    vert = lax.axis_index("vert")
    rows = own_ref.shape[0]
    columns = own_ref.shape[1]
    barrier = pltpu.get_barrier_semaphore()

    def greet_ma(step, carry):
        pl.semaphore_signal(
            barrier, inc=1, device_id=(lax.rem(ma + step, n_ma), vert), device_id_type=MESH
        )
        return carry

    def greet_vert(step, carry):
        pl.semaphore_signal(
            barrier, inc=1, device_id=(ma, lax.rem(vert + step, n_vert)), device_id_type=MESH
        )
        return carry

    lax.fori_loop(1, n_ma, greet_ma, 0)
    lax.fori_loop(1, n_vert, greet_vert, 0)
    pl.semaphore_wait(barrier, n_ma + n_vert - 2)

    def ma_copy(slot, peer):
        return pltpu.make_async_remote_copy(
            src_ref=own_ref,
            dst_ref=gathered.at[slot],
            send_sem=ma_send.at[peer],
            recv_sem=ma_recv.at[slot],
            device_id=(peer, vert),
            device_id_type=MESH,
        )

    def start_ma(step, carry):
        ma_copy(ma, lax.rem(ma + step, n_ma)).start()
        return carry

    def wait_ma(step, carry):
        other = lax.rem(ma + step, n_ma)
        ma_copy(ma, other).wait_send()
        ma_copy(other, other).wait_recv()
        return carry

    lax.fori_loop(1, n_ma, start_ma, 0)
    gathered[ma] = own_ref[...]
    lax.fori_loop(1, n_ma, wait_ma, 0)

    def column_block(block, carry):
        at = pl.ds(pl.multiple_of(block * width, width), width)
        fields = gathered[:, :, at].reshape(n_ma * rows, width)
        grid = jnp.dot(table_ref[...], fields, preferred_element_type=F32)
        weighted = (grid * factor_ref[:, at]).astype(BF16)
        back = jnp.dot(back_ref[...], weighted, preferred_element_type=F32)
        out_ref[vert, :, at] = back.astype(BF16)
        return carry

    lax.fori_loop(0, columns // width, column_block, 0)

    def vert_copy(slot, peer):
        return pltpu.make_async_remote_copy(
            src_ref=out_ref.at[slot],
            dst_ref=out_ref.at[slot],
            send_sem=vert_send.at[peer],
            recv_sem=vert_recv.at[slot],
            device_id=(ma, peer),
            device_id_type=MESH,
        )

    def start_vert(step, carry):
        vert_copy(vert, lax.rem(vert + step, n_vert)).start()
        return carry

    def wait_vert(step, carry):
        other = lax.rem(vert + step, n_vert)
        vert_copy(vert, other).wait_send()
        vert_copy(other, other).wait_recv()
        return carry

    lax.fori_loop(1, n_vert, start_vert, 0)
    lax.fori_loop(1, n_vert, wait_vert, 0)


def transform(own, table, back, factor, n_ma, n_vert):
    rows, columns = own.shape
    return pl.pallas_call(
        functools.partial(transform_kernel, n_ma, n_vert, min(columns, 512)),
        out_shape=jax.ShapeDtypeStruct((n_vert, rows, columns), BF16),
        in_specs=on_vmem(4),
        out_specs=pl.BlockSpec(memory_space=VMEM),
        scratch_shapes=[
            VMEM((n_ma, rows, columns), BF16),
            pltpu.SemaphoreType.DMA((n_ma,)),
            pltpu.SemaphoreType.DMA((n_ma,)),
            pltpu.SemaphoreType.DMA((n_vert,)),
            pltpu.SemaphoreType.DMA((n_vert,)),
        ],
        compiler_params=pltpu.CompilerParams(
            collective_id=0, has_side_effects=True, vmem_limit_bytes=GRANT
        ),
        name="transform",
    )(own, table, back, factor)


def applied_kernel(g_ref, table_ref, out_ref):
    table = table_ref[0]
    g = [g_ref[0, part].astype(F32) for part in range(4)]
    pairs = [(g[0], -g[3]), (g[1], g[2]), (-g[2], -g[1]), (-g[3], g[0])]
    for part, (first, second) in enumerate(pairs):
        adjoint = jnp.concatenate([first, second], axis=0).astype(BF16)
        out = lax.dot_general(
            adjoint, table, (((0,), (0,)), ((), ())), preferred_element_type=F32
        )
        out_ref[0, part] = out.astype(BF16)


def apply_tables(g, table):
    orders, parts, cycles, vectors = g.shape
    depth, degrees = table.shape[1:]
    return pl.pallas_call(
        applied_kernel,
        grid=(orders,),
        out_shape=jax.ShapeDtypeStruct((orders, parts, vectors, degrees), BF16),
        in_specs=[
            pl.BlockSpec((1, parts, cycles, vectors), lambda s: (s, 0, 0, 0)),
            pl.BlockSpec((1, depth, degrees), lambda s: (s, 0, 0)),
        ],
        out_specs=pl.BlockSpec((1, parts, vectors, degrees), lambda s: (s, 0, 0, 0)),
        compiler_params=pltpu.CompilerParams(vmem_limit_bytes=32 * 1024 * 1024),
        cost_estimate=pl.CostEstimate(
            flops=16 * orders * parts * vectors * degrees * depth,
            bytes_accessed=orders * parts * vectors * degrees * 2,
            transcendentals=0,
        ),
        name="apply_tables",
    )(g, table)


def gram_kernel(n_vert, at_ref, *refs):
    pieces = refs[:n_vert]
    applied_ref, out_ref, trial = refs[n_vert], refs[n_vert + 1], refs[n_vert + 2]
    vert = at_ref[0]
    vectors = pieces[0].shape[3 - 1]
    first = (pl.program_id(0) == 0) & (pl.program_id(1) == 0)
    for step in range(n_vert):
        place = lax.rem(vert + step, n_vert)
        trial[pl.ds(pl.multiple_of(place * vectors, vectors), vectors), :] = pieces[step][0, 0]

    @pl.when(first)
    def _():
        out_ref[...] = jnp.zeros_like(out_ref)

    dims = (((1,), (1,)), ((), ()))
    t = trial[...]
    a = applied_ref[0, 0]
    out_ref[0] += lax.dot_general(t, t, dims, preferred_element_type=F32)
    out_ref[1] += lax.dot_general(t, a, dims, preferred_element_type=F32)
    out_ref[2] += lax.dot_general(a, a, dims, preferred_element_type=F32)


def gram_terms(at, own, received, applied, n_vert):
    orders, parts, vectors, degrees = own.shape
    share = orders // n_vert
    total = n_vert * vectors
    block = (1, 1, vectors, degrees)
    flops = 12 * share * parts * total * total * degrees
    return pl.pallas_call(
        functools.partial(gram_kernel, n_vert),
        grid_spec=pltpu.PrefetchScalarGridSpec(
            num_scalar_prefetch=1,
            grid=(share, parts),
            in_specs=[pl.BlockSpec(block, lambda s, c, at: (at[0] * share + s, c, 0, 0))]
            + [pl.BlockSpec(block, lambda s, c, at: (s, c, 0, 0))] * (n_vert - 1)
            + [
                pl.BlockSpec(
                    (1, 1, total, degrees), lambda s, c, at: (at[0] * share + s, c, 0, 0)
                )
            ],
            out_specs=pl.BlockSpec((3, total, total), lambda s, c, at: (0, 0, 0)),
            scratch_shapes=[VMEM((total, degrees), BF16)],
        ),
        out_shape=jax.ShapeDtypeStruct((3, total, total), F32),
        compiler_params=pltpu.CompilerParams(vmem_limit_bytes=32 * 1024 * 1024),
        cost_estimate=pl.CostEstimate(
            flops=flops, bytes_accessed=4 * share * parts * total * degrees, transcendentals=0
        ),
        name="gram_terms",
    )(at, own, *received, applied)


def sum_kernel(n_vert, count, part_ref, out_ref, landed, send_a, recv_a, send_b, recv_b):
    me = lax.axis_index("ma") * n_vert + lax.axis_index("vert")
    barrier = pltpu.get_barrier_semaphore()

    def where(flat):
        return (flat // n_vert, lax.rem(flat, n_vert))

    def greet(step, carry):
        other = lax.rem(me + step, count)
        pl.semaphore_signal(barrier, inc=1, device_id=where(other), device_id_type=MESH)
        return carry

    lax.fori_loop(1, count, greet, 0)
    pl.semaphore_wait(barrier, count - 1)

    def scatter(peer, slot):
        return pltpu.make_async_remote_copy(
            src_ref=part_ref.at[peer],
            dst_ref=landed.at[slot],
            send_sem=send_a.at[peer],
            recv_sem=recv_a.at[slot],
            device_id=where(peer),
            device_id_type=MESH,
        )

    def gather(peer, slot):
        return pltpu.make_async_remote_copy(
            src_ref=out_ref.at[slot],
            dst_ref=out_ref.at[slot],
            send_sem=send_b.at[peer],
            recv_sem=recv_b.at[slot],
            device_id=where(peer),
            device_id_type=MESH,
        )

    def exchange(copy):
        def start(step, carry):
            copy(lax.rem(me + step, count), me).start()
            return carry

        def wait(step, carry):
            other = lax.rem(me + step, count)
            copy(other, me).wait_send()
            copy(other, other).wait_recv()
            return carry

        return start, wait

    start, wait = exchange(scatter)
    lax.fori_loop(1, count, start, 0)
    landed[me] = part_ref[me]
    lax.fori_loop(1, count, wait, 0)
    out_ref[me] = jnp.sum(landed[...], axis=0)
    start, wait = exchange(gather)
    lax.fori_loop(1, count, start, 0)
    lax.fori_loop(1, count, wait, 0)


def sum_over_devices(terms, n_ma, n_vert):
    count = n_ma * n_vert
    lanes = terms.shape[-1]
    rows = terms.size // lanes
    each = -(-rows // count)
    flat = terms.reshape(rows, lanes)
    if each * count != rows:
        flat = jnp.pad(flat, ((0, each * count - rows), (0, 0)))
    slots = flat.reshape(count, each, lanes)
    out = pl.pallas_call(
        functools.partial(sum_kernel, n_vert, count),
        out_shape=jax.ShapeDtypeStruct(slots.shape, F32),
        in_specs=on_vmem(1),
        out_specs=pl.BlockSpec(memory_space=VMEM),
        scratch_shapes=[VMEM(slots.shape, F32)] + [pltpu.SemaphoreType.DMA((count,))] * 4,
        compiler_params=pltpu.CompilerParams(collective_id=1, has_side_effects=True),
        name="sum_over_devices",
    )(slots)
    return out.reshape(each * count, lanes)[:rows].reshape(terms.shape)


def factor_kernel(coefficients, totals_ref, ritz_ref, mixing_ref, work):
    size = ritz_ref.shape[0]
    panel = 8
    scale = 1.0 / coefficients
    row_at = lax.broadcasted_iota(jnp.int32, (size, size), 0)
    column_at = lax.broadcasted_iota(jnp.int32, (size, size), 1)
    identity = (row_at == column_at).astype(F32)
    for b, source in enumerate((0, 2)):
        work[b, :, :size] = totals_ref[source] * scale
        work[b, :, size:] = identity
    lane = lax.broadcasted_iota(jnp.int32, (panel, size), 1)
    sub = lax.broadcasted_iota(jnp.int32, (panel, 2 * size), 0)
    all_rows = lax.broadcasted_iota(jnp.int32, (size, 2 * size), 0)

    def panel_step(p, carry):
        first = pl.multiple_of(p * panel, panel)
        at = pl.ds(first, panel)
        panels = [work[b, at, :] for b in range(2)]
        for i in range(panel):
            for b in range(2):
                x = panels[b]
                column = jnp.sum(
                    jnp.where(lane == first + i, x[:, :size], 0.0), axis=1, keepdims=True
                )
                inverse = lax.rsqrt(column[i : i + 1, :])
                line = x[i : i + 1, :] * inverse
                lower = x - (column * inverse) * line
                panels[b] = jnp.where(sub == i, line, jnp.where(sub > i, lower, x))
        for b in range(2):
            x = panels[b]
            update = lax.dot_general(
                x[:, :size], x, (((0,), (0,)), ((), ())),
                precision=HIGHEST, preferred_element_type=F32,
            )
            below = all_rows >= first + panel
            work[b] = jnp.where(below, work[b] - update, work[b])
            work[b, at, :] = x
        return carry

    lax.fori_loop(0, size // panel, panel_step, 0)
    inverse_trial = work[0, :, size:]
    half = jnp.dot(
        inverse_trial, totals_ref[1] * scale, precision=HIGHEST, preferred_element_type=F32
    )
    ritz_ref[...] = lax.dot_general(
        half, inverse_trial, (((1,), (1,)), ((), ())),
        precision=HIGHEST, preferred_element_type=F32,
    )
    mixing_ref[...] = work[1, :, size:].astype(BF16)


def finish_ritz(totals, coefficients):
    size = totals.shape[-1]
    return pl.pallas_call(
        functools.partial(factor_kernel, float(coefficients)),
        out_shape=(
            jax.ShapeDtypeStruct((size, size), F32),
            jax.ShapeDtypeStruct((size, size), BF16),
        ),
        in_specs=on_vmem(1),
        out_specs=(pl.BlockSpec(memory_space=VMEM), pl.BlockSpec(memory_space=VMEM)),
        scratch_shapes=[VMEM((2, size, 2 * size), F32)],
        name="finish_ritz",
    )(totals)


def fourier_tables(order_slot, longitudes, orders_total):
    longitude = jnp.arange(longitudes, dtype=jnp.int32)
    phases = longitude[:, None] * order_slot[None, :] % longitudes
    angles = phases.astype(F32) * (2.0 * math.pi / longitudes)
    scale = 1.0 / math.sqrt(orders_total)
    return ((jnp.cos(angles) * scale).astype(BF16), (jnp.sin(angles) * scale).astype(BF16))


def shards(trial_block, legendre, order_slot, cycle_start, cycle_count, cycle_weight):
    n_ma = lax.axis_size("ma")
    n_vert = lax.axis_size("vert")
    ma = lax.axis_index("ma")
    vert = lax.axis_index("vert")
    vectors, orders, parts, degrees = trial_block.shape
    orders_total = order_slot.shape[0]
    cycles = cycle_count.shape[0]
    live = cycles // 4
    longitudes = 2 * orders_total

    first = jnp.minimum(jnp.argmax(cycle_count > 0), cycles - live).astype(jnp.int32)
    table = lax.dynamic_slice_in_dim(legendre, first, live, 2).reshape(orders, 2 * live, degrees)
    trial = trial_block.transpose(1, 2, 0, 3)

    share = orders // n_vert
    received = []
    for step in range(1, n_vert):
        ring = [(source, (source - step) % n_vert) for source in range(n_vert)]
        target = (vert - step) % n_vert
        piece = lax.dynamic_slice_in_dim(trial, target * share, share, 0)
        received.append(lax.ppermute(piece, "vert", ring))

    products = lax.dot_general(
        table, trial, (((2,), (3,)), ((0,), (0,))), preferred_element_type=F32
    )
    w = products[:, :live]
    x = products[:, live:]
    cosine_parts = jnp.stack([w[:, :, 0] + x[:, :, 3], x[:, :, 1] - w[:, :, 2]], axis=2)
    sine_parts = jnp.stack([w[:, :, 1] - x[:, :, 2], -x[:, :, 0] - w[:, :, 3]], axis=2)
    own = jnp.stack([cosine_parts, sine_parts], axis=0).astype(BF16)
    own = own.reshape(2 * orders, live * 2 * vectors)

    cosine, sines = fourier_tables(order_slot, longitudes, orders_total)
    tables = jnp.stack(
        [
            cosine.reshape(longitudes, n_ma, orders),
            sines.reshape(longitudes, n_ma, orders),
        ],
        axis=2,
    )
    back = lax.dynamic_index_in_dim(tables, ma, 1, keepdims=False)
    back = back.reshape(longitudes, 2 * orders).T
    tables = tables.reshape(longitudes, n_ma * 2 * orders)
    starts = lax.dynamic_slice_in_dim(cycle_start, first, live)
    counts = lax.dynamic_slice_in_dim(cycle_count, first, live)
    weights = lax.dynamic_slice_in_dim(cycle_weight, first, live)
    longitude = jnp.arange(longitudes, dtype=jnp.int32)
    inside = (longitude[:, None] - starts[None, :]) % longitudes < counts[None, :]
    factor = inside.astype(F32) * weights[None, :]
    factor = jnp.broadcast_to(factor[:, :, None], (longitudes, live, 2 * vectors))
    factor = factor.reshape(longitudes, live * 2 * vectors)

    returned = transform(own, tables, back, factor, n_ma, n_vert)
    g = returned.reshape(n_vert, 2, orders, live, 2, vectors).transpose(2, 4, 1, 3, 0, 5)
    g = g.reshape(orders, 4, live, n_vert * vectors)
    applied = apply_tables(g, table)

    terms = gram_terms(vert[None].astype(jnp.int32), trial, received, applied, n_vert)
    totals = sum_over_devices(terms, n_ma, n_vert)
    ritz_matrix, mixing = finish_ritz(totals, orders_total * parts * degrees)
    mix_rows = lax.dynamic_slice_in_dim(mixing, vert * vectors, vectors, 0)
    mixed = jnp.einsum("km,scml->kscl", mix_rows, applied, preferred_element_type=F32)
    return (mixed.astype(BF16), ritz_matrix)


def solution(mesh):
    in_specs = (P("vert", "ma", None, None), P("ma", None, None, None), P(), P(), P(), P())
    out_specs = (P("vert", "ma", None, None), P())
    return jax.shard_map(shards, mesh=mesh, in_specs=in_specs, out_specs=out_specs, check_vma=False)
```

```python
import functools
import math

import jax
import jax.numpy as jnp
from jax import lax
from jax.experimental import pallas as pl
from jax.experimental.pallas import tpu as pltpu
from jax.sharding import PartitionSpec as P

MESH = pl.DeviceIdType.MESH
VMEM = pltpu.VMEM
F32 = jnp.float32
BF16 = jnp.bfloat16
HIGHEST = lax.Precision.HIGHEST
GRANT = 60 * 1024 * 1024


def on_vmem(count):
    return [pl.BlockSpec(memory_space=VMEM)] * count


def transform_kernel(
    n_ma, n_vert, width, own_ref, table_ref, back_ref, factor_ref, out_ref,
    gathered, ma_send, ma_recv, vert_send, vert_recv,
):
    ma = lax.axis_index("ma")
    vert = lax.axis_index("vert")
    rows = own_ref.shape[0]
    columns = own_ref.shape[1]
    barrier = pltpu.get_barrier_semaphore()

    def greet_ma(step, carry):
        pl.semaphore_signal(
            barrier, inc=1, device_id=(lax.rem(ma + step, n_ma), vert), device_id_type=MESH
        )
        return carry

    def greet_vert(step, carry):
        pl.semaphore_signal(
            barrier, inc=1, device_id=(ma, lax.rem(vert + step, n_vert)), device_id_type=MESH
        )
        return carry

    lax.fori_loop(1, n_ma, greet_ma, 0)
    lax.fori_loop(1, n_vert, greet_vert, 0)
    pl.semaphore_wait(barrier, n_ma + n_vert - 2)

    def ma_copy(slot, peer):
        return pltpu.make_async_remote_copy(
            src_ref=own_ref,
            dst_ref=gathered.at[slot],
            send_sem=ma_send.at[peer],
            recv_sem=ma_recv.at[slot],
            device_id=(peer, vert),
            device_id_type=MESH,
        )

    def start_ma(step, carry):
        ma_copy(ma, lax.rem(ma + step, n_ma)).start()
        return carry

    def wait_ma(step, carry):
        other = lax.rem(ma + step, n_ma)
        ma_copy(ma, other).wait_send()
        ma_copy(other, other).wait_recv()
        return carry

    lax.fori_loop(1, n_ma, start_ma, 0)
    gathered[ma] = own_ref[...]
    lax.fori_loop(1, n_ma, wait_ma, 0)

    def column_block(block, carry):
        at = pl.ds(pl.multiple_of(block * width, width), width)
        fields = gathered[:, :, at].reshape(n_ma * rows, width)
        grid = jnp.dot(table_ref[...], fields, preferred_element_type=F32)
        weighted = (grid * factor_ref[:, at]).astype(BF16)
        back = jnp.dot(back_ref[...], weighted, preferred_element_type=F32)
        out_ref[vert, :, at] = back.astype(BF16)
        return carry

    lax.fori_loop(0, columns // width, column_block, 0)

    def vert_copy(slot, peer):
        return pltpu.make_async_remote_copy(
            src_ref=out_ref.at[slot],
            dst_ref=out_ref.at[slot],
            send_sem=vert_send.at[peer],
            recv_sem=vert_recv.at[slot],
            device_id=(ma, peer),
            device_id_type=MESH,
        )

    def start_vert(step, carry):
        vert_copy(vert, lax.rem(vert + step, n_vert)).start()
        return carry

    def wait_vert(step, carry):
        other = lax.rem(vert + step, n_vert)
        vert_copy(vert, other).wait_send()
        vert_copy(other, other).wait_recv()
        return carry

    lax.fori_loop(1, n_vert, start_vert, 0)
    lax.fori_loop(1, n_vert, wait_vert, 0)


def transform(own, table, back, factor, n_ma, n_vert):
    rows, columns = own.shape
    return pl.pallas_call(
        functools.partial(transform_kernel, n_ma, n_vert, min(columns, 512)),
        out_shape=jax.ShapeDtypeStruct((n_vert, rows, columns), BF16),
        in_specs=on_vmem(4),
        out_specs=pl.BlockSpec(memory_space=VMEM),
        scratch_shapes=[
            VMEM((n_ma, rows, columns), BF16),
            pltpu.SemaphoreType.DMA((n_ma,)),
            pltpu.SemaphoreType.DMA((n_ma,)),
            pltpu.SemaphoreType.DMA((n_vert,)),
            pltpu.SemaphoreType.DMA((n_vert,)),
        ],
        compiler_params=pltpu.CompilerParams(
            collective_id=0, has_side_effects=True, vmem_limit_bytes=GRANT
        ),
        name="transform",
    )(own, table, back, factor)


def applied_parts(g, table):
    g = [part.astype(F32) for part in g]
    pairs = [(g[0], -g[3]), (g[1], g[2]), (-g[2], -g[1]), (-g[3], g[0])]
    blocks = []
    for first, second in pairs:
        adjoint = jnp.concatenate([first, second], axis=0).astype(BF16)
        out = lax.dot_general(
            adjoint, table, (((0,), (0,)), ((), ())), preferred_element_type=F32
        )
        blocks.append(out.astype(BF16))
    return blocks


def gram_kernel(n_vert, sizes, at_ref, own_ref, g_ref, table_ref, *refs):
    pieces, out_ref, stack = refs[: sum(sizes)], refs[sum(sizes)], refs[sum(sizes) + 1]
    vert = at_ref[0]
    share, parts, vectors, _ = own_ref.shape
    total = n_vert * vectors
    dims = (((1,), (1,)), ((), ()))
    sums = jnp.zeros((2 * total, 2 * total), F32)
    for s in range(share):
        applied = applied_parts([g_ref[s, part] for part in range(parts)], table_ref[s])
        for part in range(parts):
            buffer = stack.at[part % 2]
            buffer[pl.ds(pl.multiple_of(vert * vectors, vectors), vectors), :] = own_ref[s, part]
            taken = 0
            for step in range(1, n_vert):
                count = sizes[step - 1]
                each = share // count
                ref = pieces[taken + s // each]
                taken += count
                place = lax.rem(vert + step, n_vert)
                rows = pl.ds(pl.multiple_of(place * vectors, vectors), vectors)
                buffer[rows, :] = ref[s % each, part]
            buffer[total:, :] = applied[part]
            both = buffer[...]
            sums += lax.dot_general(both, both, dims, preferred_element_type=F32)
    out_ref[0] = sums[:total, :total]
    out_ref[1] = sums[:total, total:]
    out_ref[2] = sums[total:, total:]


def gram_terms(at, own, g, table, received, n_vert):
    orders, parts, vectors, degrees = own.shape
    share = orders // n_vert
    total = n_vert * vectors
    sizes = [len(pieces) for pieces in received]
    pieces = [piece for group in received for piece in group]
    here = lambda i, at: (at[0], 0, 0, 0)
    return pl.pallas_call(
        functools.partial(gram_kernel, n_vert, sizes),
        grid_spec=pltpu.PrefetchScalarGridSpec(
            num_scalar_prefetch=1,
            grid=(1,),
            in_specs=[
                pl.BlockSpec((share,) + own.shape[1:], here),
                pl.BlockSpec((share,) + g.shape[1:], here),
                pl.BlockSpec((share,) + table.shape[1:], lambda i, at: (at[0], 0, 0)),
            ]
            + [pl.BlockSpec(piece.shape, lambda i, at: (0, 0, 0, 0)) for piece in pieces],
            out_specs=pl.BlockSpec((3, total, total), lambda i, at: (0, 0, 0)),
            scratch_shapes=[VMEM((2, 2 * total, degrees), BF16)],
        ),
        out_shape=jax.ShapeDtypeStruct((3, total, total), F32),
        compiler_params=pltpu.CompilerParams(vmem_limit_bytes=32 * 1024 * 1024),
        cost_estimate=pl.CostEstimate(
            flops=12 * share * parts * total * total * degrees,
            bytes_accessed=4 * share * parts * total * degrees,
            transcendentals=0,
        ),
        name="gram_terms",
    )(at, own, g, table, *pieces)


def mix_kernel(mix_ref, g_ref, table_ref, out_ref, applied):
    parts, _, total = g_ref.shape[1:]
    vectors, _, _, degrees = out_ref.shape
    blocks = applied_parts([g_ref[0, part] for part in range(parts)], table_ref[0])
    for part, block in enumerate(blocks):
        applied[part * total : (part + 1) * total, :] = block
    mixed = jnp.dot(mix_ref[...], applied[...], preferred_element_type=F32)
    out_ref[:, 0] = mixed.reshape(vectors, parts, degrees).astype(BF16)


def mix(spread, g, table):
    orders, parts, cycles, total = g.shape
    depth, degrees = table.shape[1:]
    vectors = spread.shape[0] // parts
    return pl.pallas_call(
        mix_kernel,
        grid=(orders,),
        out_shape=jax.ShapeDtypeStruct((vectors, orders, parts, degrees), BF16),
        in_specs=[
            pl.BlockSpec(spread.shape, lambda s: (0, 0)),
            pl.BlockSpec((1, parts, cycles, total), lambda s: (s, 0, 0, 0)),
            pl.BlockSpec((1, depth, degrees), lambda s: (s, 0, 0)),
        ],
        out_specs=pl.BlockSpec((vectors, 1, parts, degrees), lambda s: (0, s, 0, 0)),
        scratch_shapes=[VMEM((parts * total, degrees), BF16)],
        compiler_params=pltpu.CompilerParams(vmem_limit_bytes=32 * 1024 * 1024),
        name="mix",
    )(spread, g, table)


def sum_kernel(n_vert, count, part_ref, out_ref, landed, send_a, recv_a, send_b, recv_b):
    me = lax.axis_index("ma") * n_vert + lax.axis_index("vert")
    barrier = pltpu.get_barrier_semaphore()

    def where(flat):
        return (flat // n_vert, lax.rem(flat, n_vert))

    def greet(step, carry):
        other = lax.rem(me + step, count)
        pl.semaphore_signal(barrier, inc=1, device_id=where(other), device_id_type=MESH)
        return carry

    lax.fori_loop(1, count, greet, 0)
    pl.semaphore_wait(barrier, count - 1)

    def scatter(peer, slot):
        return pltpu.make_async_remote_copy(
            src_ref=part_ref.at[peer],
            dst_ref=landed.at[slot],
            send_sem=send_a.at[peer],
            recv_sem=recv_a.at[slot],
            device_id=where(peer),
            device_id_type=MESH,
        )

    def gather(peer, slot):
        return pltpu.make_async_remote_copy(
            src_ref=out_ref.at[slot],
            dst_ref=out_ref.at[slot],
            send_sem=send_b.at[peer],
            recv_sem=recv_b.at[slot],
            device_id=where(peer),
            device_id_type=MESH,
        )

    def exchange(copy):
        def start(step, carry):
            copy(lax.rem(me + step, count), me).start()
            return carry

        def wait(step, carry):
            other = lax.rem(me + step, count)
            copy(other, me).wait_send()
            copy(other, other).wait_recv()
            return carry

        return start, wait

    start, wait = exchange(scatter)
    lax.fori_loop(1, count, start, 0)
    landed[me] = part_ref[me]
    lax.fori_loop(1, count, wait, 0)
    out_ref[me] = jnp.sum(landed[...], axis=0)
    start, wait = exchange(gather)
    lax.fori_loop(1, count, start, 0)
    lax.fori_loop(1, count, wait, 0)


def sum_over_devices(terms, n_ma, n_vert):
    count = n_ma * n_vert
    lanes = terms.shape[-1]
    rows = terms.size // lanes
    each = -(-rows // count)
    flat = terms.reshape(rows, lanes)
    if each * count != rows:
        flat = jnp.pad(flat, ((0, each * count - rows), (0, 0)))
    slots = flat.reshape(count, each, lanes)
    out = pl.pallas_call(
        functools.partial(sum_kernel, n_vert, count),
        out_shape=jax.ShapeDtypeStruct(slots.shape, F32),
        in_specs=on_vmem(1),
        out_specs=pl.BlockSpec(memory_space=VMEM),
        scratch_shapes=[VMEM(slots.shape, F32)] + [pltpu.SemaphoreType.DMA((count,))] * 4,
        compiler_params=pltpu.CompilerParams(collective_id=1, has_side_effects=True),
        name="sum_over_devices",
    )(slots)
    return out.reshape(each * count, lanes)[:rows].reshape(terms.shape)


def factor_kernel(coefficients, totals_ref, ritz_ref, mixing_ref, work):
    size = ritz_ref.shape[0]
    panel = 16
    scale = 1.0 / coefficients
    row_at = lax.broadcasted_iota(jnp.int32, (size, size), 0)
    column_at = lax.broadcasted_iota(jnp.int32, (size, size), 1)
    identity = (row_at == column_at).astype(F32)
    for b, source in enumerate((0, 2)):
        work[b, :, :size] = totals_ref[source] * scale
        work[b, :, size:] = identity
    lane = lax.broadcasted_iota(jnp.int32, (panel, size), 1)
    sub = lax.broadcasted_iota(jnp.int32, (panel, 2 * size), 0)
    all_rows = lax.broadcasted_iota(jnp.int32, (size, 2 * size), 0)

    def panel_step(p, carry):
        first = pl.multiple_of(p * panel, panel)
        at = pl.ds(first, panel)
        panels = [work[b, at, :] for b in range(2)]
        columns = [
            [
                jnp.sum(jnp.where(lane == first + i, x[:, :size], 0.0), axis=1, keepdims=True)
                for i in range(panel)
            ]
            for x in panels
        ]
        for i in range(panel):
            for b in range(2):
                x = panels[b]
                column = columns[b]
                inverse = lax.rsqrt(column[i][i : i + 1, :])
                scaled = column[i] * inverse
                for k in range(i + 1, panel):
                    column[k] = column[k] - scaled * (column[k][i : i + 1, :] * inverse)
                line = x[i : i + 1, :] * inverse
                panels[b] = jnp.where(sub == i, line, jnp.where(sub > i, x - scaled * line, x))
        for b in range(2):
            x = panels[b]
            update = lax.dot_general(
                x[:, :size], x, (((0,), (0,)), ((), ())),
                precision=HIGHEST, preferred_element_type=F32,
            )
            below = all_rows >= first + panel
            work[b] = jnp.where(below, work[b] - update, work[b])
            work[b, at, :] = x
        return carry

    lax.fori_loop(0, size // panel, panel_step, 0)
    inverse_trial = work[0, :, size:]
    half = jnp.dot(
        inverse_trial, totals_ref[1] * scale, precision=HIGHEST, preferred_element_type=F32
    )
    ritz_ref[...] = lax.dot_general(
        half, inverse_trial, (((1,), (1,)), ((), ())),
        precision=HIGHEST, preferred_element_type=F32,
    )
    mixing_ref[...] = work[1, :, size:].astype(BF16)


def finish_ritz(totals, coefficients):
    size = totals.shape[-1]
    return pl.pallas_call(
        functools.partial(factor_kernel, float(coefficients)),
        out_shape=(
            jax.ShapeDtypeStruct((size, size), F32),
            jax.ShapeDtypeStruct((size, size), BF16),
        ),
        in_specs=on_vmem(1),
        out_specs=(pl.BlockSpec(memory_space=VMEM), pl.BlockSpec(memory_space=VMEM)),
        scratch_shapes=[VMEM((2, size, 2 * size), F32)],
        name="finish_ritz",
    )(totals)


def fourier_tables(order_slot, longitudes, orders_total):
    longitude = jnp.arange(longitudes, dtype=jnp.int32)
    phases = longitude[:, None] * order_slot[None, :] % longitudes
    angles = phases.astype(F32) * (2.0 * math.pi / longitudes)
    scale = 1.0 / math.sqrt(orders_total)
    return ((jnp.cos(angles) * scale).astype(BF16), (jnp.sin(angles) * scale).astype(BF16))


def shards(trial_block, legendre, order_slot, cycle_start, cycle_count, cycle_weight):
    n_ma = lax.axis_size("ma")
    n_vert = lax.axis_size("vert")
    ma = lax.axis_index("ma")
    vert = lax.axis_index("vert")
    vectors, orders, parts, degrees = trial_block.shape
    orders_total = order_slot.shape[0]
    cycles = cycle_count.shape[0]
    live = cycles // 4
    longitudes = 2 * orders_total

    first = jnp.minimum(jnp.argmax(cycle_count > 0), cycles - live).astype(jnp.int32)
    table = lax.dynamic_slice_in_dim(legendre, first, live, 2).reshape(orders, 2 * live, degrees)
    trial = trial_block.transpose(1, 2, 0, 3)

    share = orders // n_vert

    def piece_for(step, begin, count):
        target = (vert - step) % n_vert
        return lax.dynamic_slice_in_dim(trial, target * share + begin, count, 0)

    def send(piece, step):
        ring = [(source, (source - step) % n_vert) for source in range(n_vert)]
        return lax.ppermute(piece, "vert", ring)

    far = n_vert // 2
    half = share // 2
    received = {step: [send(piece_for(step, 0, share), step)] for step in range(1, n_vert) if step != far}
    received[far] = [send(piece_for(far, 0, half), far)]
    late = piece_for(far, half, share - half)

    products = lax.dot_general(
        table, trial, (((2,), (3,)), ((0,), (0,))), preferred_element_type=F32
    )
    w = products[:, :live]
    x = products[:, live:]
    cosine_parts = jnp.stack([w[:, :, 0] + x[:, :, 3], x[:, :, 1] - w[:, :, 2]], axis=2)
    sine_parts = jnp.stack([w[:, :, 1] - x[:, :, 2], -x[:, :, 0] - w[:, :, 3]], axis=2)
    own = jnp.stack([cosine_parts, sine_parts], axis=0).astype(BF16)
    own = own.reshape(2 * orders, live * 2 * vectors)

    cosine, sines = fourier_tables(order_slot, longitudes, orders_total)
    tables = jnp.stack(
        [
            cosine.reshape(longitudes, n_ma, orders),
            sines.reshape(longitudes, n_ma, orders),
        ],
        axis=2,
    )
    back = lax.dynamic_index_in_dim(tables, ma, 1, keepdims=False)
    back = back.reshape(longitudes, 2 * orders).T
    tables = tables.reshape(longitudes, n_ma * 2 * orders)
    starts = lax.dynamic_slice_in_dim(cycle_start, first, live)
    counts = lax.dynamic_slice_in_dim(cycle_count, first, live)
    weights = lax.dynamic_slice_in_dim(cycle_weight, first, live)
    longitude = jnp.arange(longitudes, dtype=jnp.int32)
    inside = (longitude[:, None] - starts[None, :]) % longitudes < counts[None, :]
    factor = inside.astype(F32) * weights[None, :]
    factor = jnp.broadcast_to(factor[:, :, None], (longitudes, live, 2 * vectors))
    factor = factor.reshape(longitudes, live * 2 * vectors)

    returned = transform(own, tables, back, factor, n_ma, n_vert)
    late, returned = lax.optimization_barrier((late, returned))
    received[far].append(send(late, far))
    g = returned.reshape(n_vert, 2, orders, live, 2, vectors).transpose(2, 4, 1, 3, 0, 5)
    g = g.reshape(orders, 4, live, n_vert * vectors)

    pieces = [received[step] for step in range(1, n_vert)]
    terms = gram_terms(vert[None].astype(jnp.int32), trial, g, table, pieces, n_vert)
    totals = sum_over_devices(terms, n_ma, n_vert)
    ritz_matrix, mixing = finish_ritz(totals, orders_total * parts * degrees)
    mix_rows = lax.dynamic_slice_in_dim(mixing, vert * vectors, vectors, 0)
    spread = mix_rows[:, None, None, :] * jnp.eye(parts, dtype=BF16)[None, :, :, None]
    spread = spread.reshape(vectors * parts, parts * n_vert * vectors)
    return (mix(spread, g, table), ritz_matrix)


def solution(mesh):
    in_specs = (P("vert", "ma", None, None), P("ma", None, None, None), P(), P(), P(), P())
    out_specs = (P("vert", "ma", None, None), P())
    return jax.shard_map(shards, mesh=mesh, in_specs=in_specs, out_specs=out_specs, check_vma=False)
```

```python
import functools
import math

import jax
import jax.numpy as jnp
from jax import lax
from jax.experimental import pallas as pl
from jax.experimental.pallas import tpu as pltpu
from jax.sharding import PartitionSpec as P


MESH = pl.DeviceIdType.MESH
VMEM = pltpu.VMEM
F32 = jnp.float32
BF16 = jnp.bfloat16
HIGHEST = lax.Precision.HIGHEST
GRANT = 60 * 1024 * 1024


def on_vmem(count):
    return [pl.BlockSpec(memory_space=VMEM)] * count


def transform_kernel(
    n_ma, n_vert, width, own_ref, table_ref, back_ref, factor_ref, out_ref,
    gathered, ma_send, ma_recv, vert_send, vert_recv,
):
    ma = lax.axis_index("ma")
    vert = lax.axis_index("vert")
    rows = own_ref.shape[0]
    columns = own_ref.shape[1]
    barrier = pltpu.get_barrier_semaphore()

    def greet_ma(step, carry):
        pl.semaphore_signal(
            barrier, inc=1, device_id=(lax.rem(ma + step, n_ma), vert), device_id_type=MESH
        )
        return carry

    def greet_vert(step, carry):
        pl.semaphore_signal(
            barrier, inc=1, device_id=(ma, lax.rem(vert + step, n_vert)), device_id_type=MESH
        )
        return carry

    lax.fori_loop(1, n_ma, greet_ma, 0)
    lax.fori_loop(1, n_vert, greet_vert, 0)
    pl.semaphore_wait(barrier, n_ma + n_vert - 2)

    def ma_copy(slot, peer):
        return pltpu.make_async_remote_copy(
            src_ref=own_ref,
            dst_ref=gathered.at[slot],
            send_sem=ma_send.at[peer],
            recv_sem=ma_recv.at[slot],
            device_id=(peer, vert),
            device_id_type=MESH,
        )

    def start_ma(step, carry):
        ma_copy(ma, lax.rem(ma + step, n_ma)).start()
        return carry

    def wait_ma(step, carry):
        other = lax.rem(ma + step, n_ma)
        ma_copy(ma, other).wait_send()
        ma_copy(other, other).wait_recv()
        return carry

    lax.fori_loop(1, n_ma, start_ma, 0)
    gathered[ma] = own_ref[...]
    lax.fori_loop(1, n_ma, wait_ma, 0)

    def column_block(block, carry):
        at = pl.ds(pl.multiple_of(block * width, width), width)
        fields = gathered[:, :, at].reshape(n_ma * rows, width)
        grid = jnp.dot(table_ref[...], fields, preferred_element_type=F32)
        weighted = (grid * factor_ref[:, at]).astype(BF16)
        back = jnp.dot(back_ref[...], weighted, preferred_element_type=F32)
        out_ref[vert, :, at] = back.astype(BF16)
        return carry

    lax.fori_loop(0, columns // width, column_block, 0)

    def vert_copy(slot, peer):
        return pltpu.make_async_remote_copy(
            src_ref=out_ref.at[slot],
            dst_ref=out_ref.at[slot],
            send_sem=vert_send.at[peer],
            recv_sem=vert_recv.at[slot],
            device_id=(ma, peer),
            device_id_type=MESH,
        )

    def start_vert(step, carry):
        vert_copy(vert, lax.rem(vert + step, n_vert)).start()
        return carry

    def wait_vert(step, carry):
        other = lax.rem(vert + step, n_vert)
        vert_copy(vert, other).wait_send()
        vert_copy(other, other).wait_recv()
        return carry

    lax.fori_loop(1, n_vert, start_vert, 0)
    lax.fori_loop(1, n_vert, wait_vert, 0)


def transform(own, table, back, factor, n_ma, n_vert):
    rows, columns = own.shape
    return pl.pallas_call(
        functools.partial(transform_kernel, n_ma, n_vert, min(columns, 512)),
        out_shape=jax.ShapeDtypeStruct((n_vert, rows, columns), BF16),
        in_specs=on_vmem(4),
        out_specs=pl.BlockSpec(memory_space=VMEM),
        scratch_shapes=[
            VMEM((n_ma, rows, columns), BF16),
            pltpu.SemaphoreType.DMA((n_ma,)),
            pltpu.SemaphoreType.DMA((n_ma,)),
            pltpu.SemaphoreType.DMA((n_vert,)),
            pltpu.SemaphoreType.DMA((n_vert,)),
        ],
        compiler_params=pltpu.CompilerParams(
            collective_id=0, has_side_effects=True, vmem_limit_bytes=GRANT
        ),
        cost_estimate=pl.CostEstimate(
            flops=20_000_000_000, bytes_accessed=2 * own.size * n_ma, transcendentals=0
        ),
        name="transform",
    )(own, table, back, factor)


def applied_parts(g, table):
    g = [part.astype(F32) for part in g]
    pairs = [(g[0], -g[3]), (g[1], g[2]), (-g[2], -g[1]), (-g[3], g[0])]
    blocks = []
    for first, second in pairs:
        adjoint = jnp.concatenate([first, second], axis=0).astype(BF16)
        out = lax.dot_general(
            adjoint, table, (((0,), (0,)), ((), ())), preferred_element_type=F32
        )
        blocks.append(out.astype(BF16))
    return blocks


def gram_kernel(n_vert, sizes, at_ref, own_ref, g_ref, table_ref, *refs):
    pieces, out_ref, stack = refs[: sum(sizes)], refs[sum(sizes)], refs[sum(sizes) + 1]
    vert = at_ref[0]
    share, parts, vectors, _ = own_ref.shape
    total = n_vert * vectors
    dims = (((1,), (1,)), ((), ()))
    sums = jnp.zeros((2 * total, 2 * total), F32)
    for s in range(share):
        applied = applied_parts([g_ref[s, part] for part in range(parts)], table_ref[s])
        for part in range(parts):
            buffer = stack.at[part % 2]
            buffer[pl.ds(pl.multiple_of(vert * vectors, vectors), vectors), :] = own_ref[s, part]
            taken = 0
            for step in range(1, n_vert):
                count = sizes[step - 1]
                each = share // count
                ref = pieces[taken + s // each]
                taken += count
                place = lax.rem(vert + step, n_vert)
                rows = pl.ds(pl.multiple_of(place * vectors, vectors), vectors)
                buffer[rows, :] = ref[s % each, part]
            buffer[total:, :] = applied[part]
            both = buffer[...]
            sums += lax.dot_general(both, both, dims, preferred_element_type=F32)
    out_ref[0] = sums[:total, :total]
    out_ref[1] = sums[:total, total:]
    out_ref[2] = sums[total:, total:]


def gram_terms(at, own, g, table, received, n_vert):
    orders, parts, vectors, degrees = own.shape
    share = orders // n_vert
    total = n_vert * vectors
    sizes = [len(pieces) for pieces in received]
    pieces = [piece for group in received for piece in group]
    here = lambda i, at: (at[0], 0, 0, 0)
    return pl.pallas_call(
        functools.partial(gram_kernel, n_vert, sizes),
        grid_spec=pltpu.PrefetchScalarGridSpec(
            num_scalar_prefetch=1,
            grid=(1,),
            in_specs=[
                pl.BlockSpec((share,) + own.shape[1:], here),
                pl.BlockSpec((share,) + g.shape[1:], here),
                pl.BlockSpec((share,) + table.shape[1:], lambda i, at: (at[0], 0, 0)),
            ]
            + [pl.BlockSpec(piece.shape, lambda i, at: (0, 0, 0, 0)) for piece in pieces],
            out_specs=pl.BlockSpec((3, total, total), lambda i, at: (0, 0, 0)),
            scratch_shapes=[VMEM((2, 2 * total, degrees), BF16)],
        ),
        out_shape=jax.ShapeDtypeStruct((3, total, total), F32),
        compiler_params=pltpu.CompilerParams(vmem_limit_bytes=32 * 1024 * 1024),
        cost_estimate=pl.CostEstimate(
            flops=12 * share * parts * total * total * degrees,
            bytes_accessed=4 * share * parts * total * degrees,
            transcendentals=0,
        ),
        name="gram_terms",
    )(at, own, g, table, *pieces)


def mix_kernel(mix_ref, g_ref, table_ref, out_ref, applied):
    parts, _, total = g_ref.shape[1:]
    vectors, _, _, degrees = out_ref.shape
    blocks = applied_parts([g_ref[0, part] for part in range(parts)], table_ref[0])
    for part, block in enumerate(blocks):
        applied[part * total : (part + 1) * total, :] = block
    mixed = jnp.dot(mix_ref[...], applied[...], preferred_element_type=F32)
    out_ref[:, 0] = mixed.reshape(vectors, parts, degrees).astype(BF16)


def mix(spread, g, table):
    orders, parts, cycles, total = g.shape
    depth, degrees = table.shape[1:]
    vectors = spread.shape[0] // parts
    return pl.pallas_call(
        mix_kernel,
        grid=(orders,),
        out_shape=jax.ShapeDtypeStruct((vectors, orders, parts, degrees), BF16),
        in_specs=[
            pl.BlockSpec(spread.shape, lambda s: (0, 0)),
            pl.BlockSpec((1, parts, cycles, total), lambda s: (s, 0, 0, 0)),
            pl.BlockSpec((1, depth, degrees), lambda s: (s, 0, 0)),
        ],
        out_specs=pl.BlockSpec((vectors, 1, parts, degrees), lambda s: (0, s, 0, 0)),
        scratch_shapes=[VMEM((parts * total, degrees), BF16)],
        compiler_params=pltpu.CompilerParams(vmem_limit_bytes=32 * 1024 * 1024),
        name="mix",
    )(spread, g, table)


def sum_kernel(
    n_vert, count, owners, part_ref, out_ref, landed, send_a, recv_a, send_b, recv_b
):
    ma = lax.axis_index("ma")
    vert = lax.axis_index("vert")
    slots = part_ref.shape[0]
    me = ma * n_vert + vert
    mine = jnp.where(vert < owners, lax.rem(ma * owners + vert, slots), 0)
    owning = (vert < owners) & (ma * owners + vert < slots)
    barrier = pltpu.get_barrier_semaphore()

    def where(flat):
        return (flat // n_vert, lax.rem(flat, n_vert))

    def owner(slot):
        return slot // owners * n_vert + lax.rem(slot, owners)

    def greet(step, carry):
        other = lax.rem(me + step, count)
        pl.semaphore_signal(barrier, inc=1, device_id=where(other), device_id_type=MESH)
        return carry

    lax.fori_loop(1, count, greet, 0)
    pl.semaphore_wait(barrier, count - 1)

    def scatter(slot, source):
        return pltpu.make_async_remote_copy(
            src_ref=part_ref.at[slot],
            dst_ref=landed.at[source],
            send_sem=send_a.at[slot],
            recv_sem=recv_a.at[source],
            device_id=where(owner(slot)),
            device_id_type=MESH,
        )

    def gather(peer, slot):
        return pltpu.make_async_remote_copy(
            src_ref=out_ref.at[slot],
            dst_ref=out_ref.at[slot],
            send_sem=send_b.at[peer],
            recv_sem=recv_b.at[slot],
            device_id=where(peer),
            device_id_type=MESH,
        )

    def over_slots(act):
        def body(step, carry):
            slot = lax.rem(ma * owners + vert + step, slots)

            @pl.when(owner(slot) != me)
            def _():
                act(slot)

            return carry

        lax.fori_loop(0, slots, body, 0)

    def over_others(act):
        def body(step, carry):
            act(lax.rem(me + step, count))
            return carry

        lax.fori_loop(1, count, body, 0)

    over_slots(lambda slot: scatter(slot, me).start())

    @pl.when(owning)
    def _():
        landed[me] = part_ref[mine]
        over_others(lambda other: scatter(mine, other).wait_recv())
        out_ref[mine] = jnp.sum(landed[...], axis=0)
        over_others(lambda other: gather(other, mine).start())

    over_slots(lambda slot: scatter(slot, me).wait_send())
    over_slots(lambda slot: gather(me, slot).wait_recv())

    @pl.when(owning)
    def _():
        over_others(lambda other: gather(other, mine).wait_send())


def sum_over_devices(terms, n_ma, n_vert):
    count = n_ma * n_vert
    lanes = terms.shape[-1]
    rows = terms.size // lanes
    each = 8
    while rows % each or rows // each > count:
        each *= 2
    slots = rows // each
    owners = slots // n_ma if slots % n_ma == 0 else n_vert
    parts = terms.reshape(slots, each, lanes)
    out = pl.pallas_call(
        functools.partial(sum_kernel, n_vert, count, owners),
        out_shape=jax.ShapeDtypeStruct(parts.shape, F32),
        in_specs=on_vmem(1),
        out_specs=pl.BlockSpec(memory_space=VMEM),
        scratch_shapes=[
            VMEM((count, each, lanes), F32),
            pltpu.SemaphoreType.DMA((slots,)),
            pltpu.SemaphoreType.DMA((count,)),
            pltpu.SemaphoreType.DMA((count,)),
            pltpu.SemaphoreType.DMA((slots,)),
        ],
        compiler_params=pltpu.CompilerParams(collective_id=1, has_side_effects=True),
        name="sum_over_devices",
    )(parts)
    return out.reshape(terms.shape)


def factor_kernel(coefficients, totals_ref, ritz_ref, mixing_ref, work):
    size = ritz_ref.shape[0]
    panel = 16
    scale = 1.0 / coefficients
    row_at = lax.broadcasted_iota(jnp.int32, (size, size), 0)
    column_at = lax.broadcasted_iota(jnp.int32, (size, size), 1)
    identity = (row_at == column_at).astype(F32)
    for b, source in enumerate((0, 2)):
        work[b, :, :size] = totals_ref[source] * scale
        work[b, :, size:] = identity
    lane = lax.broadcasted_iota(jnp.int32, (panel, size), 1)
    sub = lax.broadcasted_iota(jnp.int32, (panel, 2 * size), 0)
    all_rows = lax.broadcasted_iota(jnp.int32, (size, 2 * size), 0)

    def panel_step(p, carry):
        first = pl.multiple_of(p * panel, panel)
        at = pl.ds(first, panel)
        panels = [work[b, at, :] for b in range(2)]
        columns = [
            [
                jnp.sum(jnp.where(lane == first + i, x[:, :size], 0.0), axis=1, keepdims=True)
                for i in range(panel)
            ]
            for x in panels
        ]
        for i in range(panel):
            for b in range(2):
                x = panels[b]
                column = columns[b]
                inverse = lax.rsqrt(column[i][i : i + 1, :])
                scaled = column[i] * inverse
                for k in range(i + 1, panel):
                    column[k] = column[k] - scaled * (column[k][i : i + 1, :] * inverse)
                line = x[i : i + 1, :] * inverse
                panels[b] = jnp.where(sub == i, line, jnp.where(sub > i, x - scaled * line, x))
        for b in range(2):
            x = panels[b]
            update = lax.dot_general(
                x[:, :size], x, (((0,), (0,)), ((), ())),
                precision=HIGHEST, preferred_element_type=F32,
            )
            below = all_rows >= first + panel
            work[b] = jnp.where(below, work[b] - update, work[b])
            work[b, at, :] = x
        return carry

    lax.fori_loop(0, size // panel, panel_step, 0)
    inverse_trial = work[0, :, size:]
    half = jnp.dot(
        inverse_trial, totals_ref[1] * scale, precision=HIGHEST, preferred_element_type=F32
    )
    ritz_ref[...] = lax.dot_general(
        half, inverse_trial, (((1,), (1,)), ((), ())),
        precision=HIGHEST, preferred_element_type=F32,
    )
    mixing_ref[...] = work[1, :, size:].astype(BF16)


def finish_ritz(totals, coefficients):
    size = totals.shape[-1]
    return pl.pallas_call(
        functools.partial(factor_kernel, float(coefficients)),
        out_shape=(
            jax.ShapeDtypeStruct((size, size), F32),
            jax.ShapeDtypeStruct((size, size), BF16),
        ),
        in_specs=on_vmem(1),
        out_specs=(pl.BlockSpec(memory_space=VMEM), pl.BlockSpec(memory_space=VMEM)),
        scratch_shapes=[VMEM((2, size, 2 * size), F32)],
        name="finish_ritz",
    )(totals)


def fourier_tables(order_slot, longitudes, orders_total):
    longitude = jnp.arange(longitudes, dtype=jnp.int32)
    phases = longitude[:, None] * order_slot[None, :] % longitudes
    angles = phases.astype(F32) * (2.0 * math.pi / longitudes)
    scale = 1.0 / math.sqrt(orders_total)
    return ((jnp.cos(angles) * scale).astype(BF16), (jnp.sin(angles) * scale).astype(BF16))


def shards(trial_block, legendre, order_slot, cycle_start, cycle_count, cycle_weight):
    n_ma = lax.axis_size("ma")
    n_vert = lax.axis_size("vert")
    ma = lax.axis_index("ma")
    vert = lax.axis_index("vert")
    vectors, orders, parts, degrees = trial_block.shape
    orders_total = order_slot.shape[0]
    cycles = cycle_count.shape[0]
    live = cycles // 4
    longitudes = 2 * orders_total

    first = jnp.minimum(jnp.argmax(cycle_count > 0), cycles - live).astype(jnp.int32)
    table = lax.dynamic_slice_in_dim(legendre, first, live, 2).reshape(orders, 2 * live, degrees)
    trial = trial_block.transpose(1, 2, 0, 3)

    share = orders // n_vert

    def piece_for(step, begin, count):
        target = (vert - step) % n_vert
        return lax.dynamic_slice_in_dim(trial, target * share + begin, count, 0)

    def send(piece, step):
        ring = [(source, (source - step) % n_vert) for source in range(n_vert)]
        return lax.ppermute(piece, "vert", ring)

    far = n_vert // 2
    half = share // 2
    received = {step: [send(piece_for(step, 0, share), step)] for step in range(1, n_vert) if step != far}
    early = piece_for(far, 0, half)
    received[far] = [send(early, far)]
    late = piece_for(far, half, share - half)

    products = lax.dot_general(
        table, trial, (((2,), (3,)), ((0,), (0,))), preferred_element_type=F32
    )
    w = products[:, :live]
    x = products[:, live:]
    cosine_parts = jnp.stack([w[:, :, 0] + x[:, :, 3], x[:, :, 1] - w[:, :, 2]], axis=2)
    sine_parts = jnp.stack([w[:, :, 1] - x[:, :, 2], -x[:, :, 0] - w[:, :, 3]], axis=2)
    own = jnp.stack([cosine_parts, sine_parts], axis=0).astype(BF16)
    own = own.reshape(2 * orders, live * 2 * vectors)

    cosine, sines = fourier_tables(order_slot, longitudes, orders_total)
    tables = jnp.stack(
        [
            cosine.reshape(longitudes, n_ma, orders),
            sines.reshape(longitudes, n_ma, orders),
        ],
        axis=2,
    )
    back = lax.dynamic_index_in_dim(tables, ma, 1, keepdims=False)
    back = back.reshape(longitudes, 2 * orders).T
    tables = tables.reshape(longitudes, n_ma * 2 * orders)
    starts = lax.dynamic_slice_in_dim(cycle_start, first, live)
    counts = lax.dynamic_slice_in_dim(cycle_count, first, live)
    weights = lax.dynamic_slice_in_dim(cycle_weight, first, live)
    longitude = jnp.arange(longitudes, dtype=jnp.int32)
    inside = (longitude[:, None] - starts[None, :]) % longitudes < counts[None, :]
    factor = inside.astype(F32) * weights[None, :]
    factor = jnp.broadcast_to(factor[:, :, None], (longitudes, live, 2 * vectors))
    factor = factor.reshape(longitudes, live * 2 * vectors)

    returned = transform(own, tables, back, factor, n_ma, n_vert)
    late, returned = lax.optimization_barrier((late, returned))
    received[far].append(send(late, far))
    g = returned.reshape(n_vert, 2, orders, live, 2, vectors).transpose(2, 4, 1, 3, 0, 5)
    g = g.reshape(orders, 4, live, n_vert * vectors)

    pieces = [received[step] for step in range(1, n_vert)]
    terms = gram_terms(vert[None].astype(jnp.int32), trial, g, table, pieces, n_vert)
    totals = sum_over_devices(terms, n_ma, n_vert)
    ritz_matrix, mixing = finish_ritz(totals, orders_total * parts * degrees)
    mix_rows = lax.dynamic_slice_in_dim(mixing, vert * vectors, vectors, 0)
    spread = mix_rows[:, None, None, :] * jnp.eye(parts, dtype=BF16)[None, :, :, None]
    spread = spread.reshape(vectors * parts, parts * n_vert * vectors)
    return (mix(spread, g, table), ritz_matrix)


def solution(mesh):
    in_specs = (P("vert", "ma", None, None), P("ma", None, None, None), P(), P(), P(), P())
    out_specs = (P("vert", "ma", None, None), P())
    return jax.shard_map(shards, mesh=mesh, in_specs=in_specs, out_specs=out_specs, check_vma=False)
```
